128 devices in a mesh: data: 1, time: 128 (over z, y, x, core).
Axes of the slice: x: 4, y: 4, z: 4, core: 2. Of those that a mesh axis runs over, the one named last changes fastest.
Arguments:
- x_init: float32 [2, 64, 768], P('data')
- w_in: bfloat16 [768, 3072], replicated
- w_out: bfloat16 [3072, 768], replicated
- gamma_c: bfloat16 [1536, 3072], P('time')
- beta_c: bfloat16 [1536, 3072], P('time')
- gamma_u: bfloat16 [1536, 3072], P('time')
- beta_u: bfloat16 [1536, 3072], P('time')
- step_h: float32 [1536], P('time')
- guide_w: float32 [1], replicated
Outputs:
- output: float32 [1536, 2, 64, 768], P('time', 'data')
All inputs are finite; a program needn't handle non-finite values.
Results may differ from the reference program's by a relative error of at most 0.00877005.
Values are sent between devices in bfloat16 or wider.
A program may use at most 1 GiB of HBM per device.

```python
import jax
import jax.numpy as jnp
from jax import lax

SAMPLES = 2
TOKENS = 64
CHANNELS = 768
HIDDEN = 3072
NUM_STEPS = 1536
NUM_SWEEPS = 4


def setup_inputs(seed: int = 0, part: int = 0) -> dict:
    base_key = jax.random.key(seed)
    part_key = jax.random.fold_in(base_key, part)
    sub_keys = jax.random.split(base_key, 8)
    x_init = jax.random.normal(part_key, (SAMPLES, TOKENS, CHANNELS), jnp.float32)
    w_in = (jax.random.normal(sub_keys[0], (CHANNELS, HIDDEN), jnp.float32) * CHANNELS ** -0.5).astype(jnp.bfloat16)
    w_out = (jax.random.normal(sub_keys[1], (HIDDEN, CHANNELS), jnp.float32) * HIDDEN ** -0.5).astype(jnp.bfloat16)
    gamma_c = (0.5 * jax.random.normal(sub_keys[2], (NUM_STEPS, HIDDEN), jnp.float32)).astype(jnp.bfloat16)
    beta_c = (0.5 * jax.random.normal(sub_keys[3], (NUM_STEPS, HIDDEN), jnp.float32)).astype(jnp.bfloat16)
    gamma_u = (0.5 * jax.random.normal(sub_keys[4], (NUM_STEPS, HIDDEN), jnp.float32)).astype(jnp.bfloat16)
    beta_u = (0.5 * jax.random.normal(sub_keys[5], (NUM_STEPS, HIDDEN), jnp.float32)).astype(jnp.bfloat16)
    step_h = jax.random.normal(sub_keys[6], (NUM_STEPS,), jnp.float32) * (0.6 * NUM_STEPS ** -0.5)
    guide_w = jax.random.uniform(sub_keys[7], (1,), jnp.float32, 1.0, 3.0)
    return {"x_init": x_init, "w_in": w_in, "w_out": w_out, "gamma_c": gamma_c, "beta_c": beta_c, "gamma_u": gamma_u, "beta_u": beta_u, "step_h": step_h, "guide_w": guide_w}


def reference(x_init, w_in, w_out, gamma_c, beta_c, gamma_u, beta_u, step_h, guide_w):
    guide = guide_w[0]
    tok_rows = SAMPLES * TOKENS

    def one_step(step_args):
        x_step, cond_gain, cond_shift, unc_gain, unc_shift, h_one = step_args
        pre_act = jnp.dot(x_step.reshape(tok_rows, CHANNELS).astype(jnp.bfloat16), w_in, preferred_element_type=jnp.float32)
        act_c = jax.nn.gelu(pre_act * (1.0 + cond_gain.astype(jnp.float32)) + cond_shift.astype(jnp.float32)).astype(jnp.bfloat16)
        act_u = jax.nn.gelu(pre_act * (1.0 + unc_gain.astype(jnp.float32)) + unc_shift.astype(jnp.float32)).astype(jnp.bfloat16)
        out_c = jnp.dot(act_c, w_out, preferred_element_type=jnp.float32)
        out_u = jnp.dot(act_u, w_out, preferred_element_type=jnp.float32)
        drift = h_one * ((1.0 + guide) * out_c - guide * out_u)
        return drift.reshape(SAMPLES, TOKENS, CHANNELS)

    def sweep(states, unused):
        drifts = lax.map(one_step, (states, gamma_c, beta_c, gamma_u, beta_u, step_h))
        earlier = jnp.cumsum(drifts[:-1], axis=0)
        offsets = jnp.concatenate([jnp.zeros_like(drifts[:1]), earlier], axis=0)
        return x_init[None] + offsets, None

    start = jnp.broadcast_to(x_init[None], (NUM_STEPS, SAMPLES, TOKENS, CHANNELS))
    final, ignored = lax.scan(sweep, start, None, length=NUM_SWEEPS)
    return final
```

```python
import functools
import math

import jax
import jax.numpy as jnp
from jax import lax
from jax.experimental import pallas as pl
from jax.experimental.pallas import tpu as pltpu
from jax.sharding import PartitionSpec as P

NUM_SWEEPS = 4
CHUNKS = 4
HID_TILE = 256
MESH = pl.DeviceIdType.MESH
GELU_SLOPE = 2.0 * math.sqrt(2.0 / math.pi)
GELU_CUBIC = 4.0 * GELU_SLOPE * 0.044715


def gelu_of_half(half):
    inner = half * (half * half * GELU_CUBIC + GELU_SLOPE)
    return half + half * jnp.tanh(inner)


def sampler(dims, x_ref, w_in, w_out, gamma_c, beta_c, gamma_u, beta_u, step_ref, guide_ref, out_ref,
            local, sib_local, before, sib_before, state, act, first_pre, gains, sib_mod, coef, own_coef, sib_coef,
            tx, rx, send_sem, recv_sem, mod_send, mod_recv, coef_send, coef_recv, loc_send, loc_recv, bef_send, bef_recv):
    steps, rows, channels, hidden, side = dims
    both = 2 * steps
    tall = both * rows
    index = lax.axis_index("time")
    core = lax.rem(index, 2)
    chip = lax.div(index, 2)
    sibling = index + 1 - 2 * core
    coords = (lax.rem(chip, side), lax.rem(lax.div(chip, side), side), lax.div(chip, side * side))
    strides = (2, 2 * side, 2 * side * side)

    def at(target):
        return {"time": target}

    def peer(phase, hop):
        return index + (lax.rem(coords[phase] + hop, side) - coords[phase]) * strides[phase]

    barrier = pltpu.get_barrier_semaphore()
    pl.semaphore_signal(barrier, inc=1, device_id=at(sibling), device_id_type=MESH)
    for phase in range(3):
        for hop in range(1, side):
            pl.semaphore_signal(barrier, inc=1, device_id=at(peer(phase, hop)), device_id_type=MESH)
    pl.semaphore_wait(barrier, 1 + 3 * (side - 1))

    mods = (gamma_c, beta_c, gamma_u, beta_u)
    mod_copies = [pltpu.make_async_remote_copy(src_ref=mods[i], dst_ref=sib_mod.at[i], send_sem=mod_send.at[i], recv_sem=mod_recv.at[i], device_id=at(sibling), device_id_type=MESH) for i in range(4)]
    for copy in mod_copies:
        copy.start()
    guide = guide_ref[0]
    for j in range(steps):
        own_coef[0, j:j + 1, :] = jnp.full((1, channels), step_ref[j] * (1.0 + guide), jnp.float32)
        own_coef[1, j:j + 1, :] = jnp.full((1, channels), step_ref[j] * guide, jnp.float32)
    coef_copy = pltpu.make_async_remote_copy(src_ref=own_coef, dst_ref=sib_coef, send_sem=coef_send, recv_sem=coef_recv, device_id=at(sibling), device_id_type=MESH)

    x_rows = x_ref[core].astype(jnp.bfloat16)
    for tile in range(hidden // HID_TILE):
        cols = slice(tile * HID_TILE, (tile + 1) * HID_TILE)
        first_pre[:, cols] = jnp.dot(x_rows, w_in[:, cols], preferred_element_type=jnp.float32)
    coef_copy.start()

    first = core == 0
    for copy in mod_copies:
        copy.wait()
    for i in range(4):
        mine = mods[i][...].astype(jnp.float32)
        theirs = sib_mod[i].astype(jnp.float32)
        if i % 2 == 0:
            mine, theirs = 0.5 + 0.5 * mine, 0.5 + 0.5 * theirs
        else:
            mine, theirs = 0.5 * mine, 0.5 * theirs
        gains[i, 0:steps, :] = jnp.where(first, mine, theirs)
        gains[i, steps:both, :] = jnp.where(first, theirs, mine)
    coef_copy.wait()
    for i in range(2):
        coef[i, 0:steps, :] = jnp.where(first, own_coef[i], sib_coef[i])
        coef[i, steps:both, :] = jnp.where(first, sib_coef[i], own_coef[i])

    def copies(phase, chunk, turn):
        return [pltpu.make_async_remote_copy(
            src_ref=tx.at[phase, turn], dst_ref=rx.at[phase, chunk, hop - 1], send_sem=send_sem.at[phase, turn, hop - 1],
            recv_sem=recv_sem.at[phase, chunk, hop - 1], device_id=at(peer(phase, hop)), device_id_type=MESH) for hop in range(1, side)]

    def send(phase, chunk, turn):
        for copy in copies(phase, chunk, turn):
            copy.start()

    def finish(phase, chunk, turn):
        for copy in copies(phase, chunk, turn):
            copy.wait()
        lower = jnp.zeros((rows, channels), jnp.float32)
        total = tx[phase, turn]
        for hop in range(1, side):
            part = rx[phase, chunk, hop - 1]
            total = total + part
            lower = lower + jnp.where(coords[phase] >= hop, part, 0.0)
        before[chunk] = lower if phase == 0 else before[chunk] + lower
        if phase < 2:
            tx[phase + 1, turn] = total
            send(phase + 1, chunk, turn)

    def drifts(chunk):
        outs = jnp.dot(act[...], w_out[...], preferred_element_type=jnp.float32)
        run = jnp.zeros((rows, channels), jnp.float32)
        for j in range(both):
            local[chunk, j] = run
            run = run + (outs[j * rows:(j + 1) * rows] * coef[0, j:j + 1, :] - outs[tall + j * rows:tall + (j + 1) * rows] * coef[1, j:j + 1, :])
        return run

    def activate(pre, j, cols):
        for branch in range(2):
            half = pre * gains[2 * branch, j:j + 1, cols] + gains[2 * branch + 1, j:j + 1, cols]
            start = branch * tall + j * rows
            act[start:start + rows, cols] = gelu_of_half(half).astype(jnp.bfloat16)

    def exchange(turn_now, last, step_index):
        for phase in range(3):
            lag = phase + 1

            def one(phase=phase, lag=lag):
                older = step_index - lag
                finish(phase, lax.rem(older, CHUNKS), lax.rem(older, 2))
            if last:
                one()
            else:
                pl.when(step_index >= lag)(one)

    def first_chunk(step_index, carry):
        chunk = step_index
        turn = lax.rem(step_index, 2)
        top = pl.multiple_of(chunk * rows, rows)
        for tile in range(hidden // HID_TILE):
            cols = slice(tile * HID_TILE, (tile + 1) * HID_TILE)
            pre = first_pre[pl.ds(top, rows), cols]
            for j in range(both):
                activate(pre, j, cols)
        tx[0, turn] = drifts(chunk)
        send(0, chunk, turn)
        exchange(turn, False, step_index)
        return carry

    def later_chunk(step_index, carry):
        chunk = lax.rem(step_index, CHUNKS)
        turn = lax.rem(step_index, 2)
        top = pl.multiple_of(chunk * rows, rows)
        base = x_ref[core, pl.ds(top, rows), :] + before[chunk]
        for j in range(both):
            state[j * rows:(j + 1) * rows, :] = (base + local[chunk, j]).astype(jnp.bfloat16)
        for tile in range(hidden // HID_TILE):
            cols = slice(tile * HID_TILE, (tile + 1) * HID_TILE)
            pre = jnp.dot(state[...], w_in[:, cols], preferred_element_type=jnp.float32)
            for j in range(both):
                activate(pre[j * rows:(j + 1) * rows], j, cols)
        tx[0, turn] = drifts(chunk)
        send(0, chunk, turn)
        exchange(turn, True, step_index)
        return carry

    lax.fori_loop(0, CHUNKS, first_chunk, 0)
    lax.fori_loop(CHUNKS, NUM_SWEEPS * CHUNKS, later_chunk, 0)

    def local_copy(chunk):
        return pltpu.make_async_remote_copy(
            src_ref=local.at[chunk, pl.ds((1 - core) * steps, steps)], dst_ref=sib_local.at[chunk], send_sem=loc_send.at[chunk],
            recv_sem=loc_recv.at[chunk], device_id=at(sibling), device_id_type=MESH)

    def before_copy(chunk):
        return pltpu.make_async_remote_copy(
            src_ref=before.at[chunk], dst_ref=sib_before.at[chunk], send_sem=bef_send.at[chunk],
            recv_sem=bef_recv.at[chunk], device_id=at(sibling), device_id_type=MESH)

    def give(chunk):
        span = slice(chunk * rows, (chunk + 1) * rows)
        local_copy(chunk).wait()
        before_copy(chunk).wait()
        mine = x_ref[core, span, :] + before[chunk]
        theirs = x_ref[1 - core, span, :] + sib_before[chunk]
        for j in range(steps):
            out_ref[j, core, span, :] = mine + local[chunk, core * steps + j]
            out_ref[j, 1 - core, span, :] = theirs + sib_local[chunk, j]

    for chunk in range(CHUNKS):
        local_copy(chunk).start()
    before_copy(0).start()
    finish(0, 3, 1)
    finish(1, 2, 0)
    finish(2, 1, 1)
    before_copy(1).start()
    give(0)
    finish(1, 3, 1)
    finish(2, 2, 0)
    before_copy(2).start()
    give(1)
    give(2)
    finish(2, 3, 1)
    before_copy(3).start()
    give(3)


def solution(mesh):
    num_time = mesh.shape["time"]
    side = round((num_time // 2) ** (1 / 3))

    def body(x_init, w_in, w_out, gamma_c, beta_c, gamma_u, beta_u, step_h, guide_w):
        samples, tokens, channels = x_init.shape
        hidden = w_in.shape[1]
        steps = step_h.shape[0]
        rows = tokens // CHUNKS
        both = 2 * steps
        f32, bf16 = jnp.float32, jnp.bfloat16
        vmem = pl.BlockSpec(memory_space=pltpu.VMEM)
        smem = pl.BlockSpec(memory_space=pltpu.SMEM)
        dma = pltpu.SemaphoreType.DMA
        hops = side - 1
        return pl.pallas_call(
            functools.partial(sampler, (steps, rows, channels, hidden, side)),
            out_shape=jax.ShapeDtypeStruct((steps, samples, tokens, channels), f32),
            in_specs=[vmem] * 7 + [smem] * 2,
            out_specs=vmem,
            scratch_shapes=[
                pltpu.VMEM((CHUNKS, both, rows, channels), f32),
                pltpu.VMEM((CHUNKS, steps, rows, channels), f32),
                pltpu.VMEM((CHUNKS, rows, channels), f32),
                pltpu.VMEM((CHUNKS, rows, channels), f32),
                pltpu.VMEM((both * rows, channels), bf16),
                pltpu.VMEM((2 * both * rows, hidden), bf16),
                pltpu.VMEM((tokens, hidden), f32),
                pltpu.VMEM((4, both, hidden), f32),
                pltpu.VMEM((4, steps, hidden), bf16),
                pltpu.VMEM((2, both, channels), f32),
                pltpu.VMEM((2, steps, channels), f32),
                pltpu.VMEM((2, steps, channels), f32),
                pltpu.VMEM((3, 2, rows, channels), f32),
                pltpu.VMEM((3, CHUNKS, hops, rows, channels), f32),
                dma((3, 2, hops)), dma((3, CHUNKS, hops)),
                dma((4,)), dma((4,)), dma, dma,
                dma((CHUNKS,)), dma((CHUNKS,)), dma((CHUNKS,)), dma((CHUNKS,)),
            ],
            compiler_params=pltpu.CompilerParams(collective_id=0, has_side_effects=True, vmem_limit_bytes=62 * 2 ** 20),
            name="picard_sampler",
        )(x_init, w_in, w_out, gamma_c, beta_c, gamma_u, beta_u, step_h, guide_w)

    return jax.shard_map(body, mesh=mesh, in_specs=(P("data", None, None), P(None, None), P(None, None), P("time", None), P("time", None), P("time", None), P("time", None), P("time"), P(None)), out_specs=P("time", "data", None, None), check_vma=False)
```
